512 devices in a mesh: lon: 8 (over x, core), lat: 16 (over z), lev: 4 (over y).
Axes of the slice: x: 4, y: 4, z: 16, core: 2. Of those that a mesh axis runs over, the one named last changes fastest.
Arguments:
- solution: float32 [36, 8, 128, 1024], P(None, 'lev', 'lat', 'lon'), may hold values from -6 to 6
- residual: float32 [36, 8, 128, 1024], P(None, 'lev', 'lat', 'lon'), may hold values from -24 to 24
- direction: float32 [36, 8, 128, 1024], P(None, 'lev', 'lat', 'lon'), may hold values from -24 to 24
- ensemble: bfloat16 [32, 4, 8, 128, 1024], P(None, None, 'lev', 'lat', 'lon'), may hold values from -6 to 6
- static_sd: float32 [4, 8, 128, 1024], P(None, 'lev', 'lat', 'lon'), may hold values from 0.5 to 2
- send_tile: int32 [4, 8, 16, 128, 2], P('lev', 'lon', 'lat'), may hold values from 0 to 15
- pair_count: int32 [4, 8, 16, 128], P('lev', 'lon', 'lat'), may hold values from 1 to 2, as said below
- obs_weight: bfloat16 [4, 8, 16, 128, 2, 8, 512], P('lev', 'lon', 'lat'), may hold values from -0.25 to 0.25
- obs_precision: float32 [4, 8, 16, 128, 2, 8], P('lev', 'lon', 'lat'), may hold values from 100 to 3000
Outputs:
- new_solution: float32 [36, 8, 128, 1024], P(None, 'lev', 'lat', 'lon')
- new_residual: float32 [36, 8, 128, 1024], P(None, 'lev', 'lat', 'lon')
- new_direction: float32 [36, 8, 128, 1024], P(None, 'lev', 'lat', 'lon')
The draws below stay inside these ranges and needn't reach their ends.
Inputs may be any that keep to these rules, and one draw needn't show every extreme that they name: `pair_count`: every device sends at least one and at most 2 live slots to every owner of its level plane; in every level plane some owner has 2 live slots from every device of the plane.
All inputs are finite; a program needn't handle non-finite values.
Results may differ from the reference program's by a relative error of at most 0.0034.
Values may be sent and summed in bfloat16 or wider, within the bound.
No kernel may reach another device: no remote copies, remote signals or barrier semaphores. Data moves between devices by JAX's collectives and lax.ppermute only.
A program may use at most 64 MiB of HBM per device.

```python
import math
import jax
import jax.numpy as jnp
from jax import lax

MEMBERS = 32
VARS = 4
CLEV = 2
CLAT = 8
CLON = 128
SLOTS = 2
OBS = 8
FIELDS = 36
TILES = 16
GROUP = 128
NLEV = 8
NLAT = 128
NLON = 1024
N_LON = 8
N_LAT = 16
N_LEV = 4


def scaled_field(key, reverse):
    key_list = jax.random.split(key, 3)
    field_scale = jnp.exp(jax.random.uniform(key_list[0], (FIELDS, 1, 1, 1), jnp.float32, 0.0, jnp.log(2.0)))
    row_scale = jnp.exp(jax.random.uniform(key_list[1], (1, NLEV, NLAT, 1), jnp.float32, 0.0, jnp.log(2.0)))
    lon_ramp = jnp.arange(NLON, dtype=jnp.float32) / NLON
    if reverse:
        lon_ramp = 1.0 - lon_ramp
    lon_scale = jnp.exp(jnp.log(3.0) * lon_ramp).reshape(1, 1, 1, NLON)
    scale_field = 0.5 * field_scale * row_scale * lon_scale
    noise_field = jnp.clip(jax.random.normal(key_list[2], (FIELDS, NLEV, NLAT, NLON), jnp.float32), -4.0, 4.0)
    return noise_field * scale_field


def draw_residual(key, part):
    return scaled_field(jax.random.fold_in(key, 11), False)


def draw_direction(key, part):
    return scaled_field(jax.random.fold_in(key, 23), True)


def draw_pair_count(key, part):
    key_list = jax.random.split(jax.random.fold_in(key, 37), 3)
    base_count = jax.random.randint(key_list[0], (N_LEV, N_LON, N_LAT, GROUP), 1, SLOTS + 1)
    owner_limit = jax.random.randint(key_list[1], (N_LEV, 1, 1, GROUP), 1, SLOTS + 1)
    base_count = jnp.minimum(base_count, owner_limit)
    busiest = jax.random.randint(key_list[2], (N_LEV, 1, 1, 1), 0, GROUP)
    column = jnp.arange(GROUP, dtype=jnp.int32).reshape(1, 1, 1, GROUP)
    return jnp.where(column == busiest, SLOTS, base_count).astype(jnp.int32)


def plant(drawn, rng, least, largest):
    place = [jax.random.randint(jax.random.fold_in(rng, axis), (), 0, length) for axis, length in enumerate(drawn.shape)]
    widest = drawn.shape.index(max(drawn.shape))
    next_to = place[:widest] + [(place[widest] + 1) % drawn.shape[widest]] + place[widest + 1:]
    return drawn.at[tuple(place)].set(least).at[tuple(next_to)].set(largest)


def steps_of(key, shape, pieces, low, top_value):
    loudness, own = 1.0, jax.random.fold_in(key, 6)
    for position, parts in pieces:
        heights = jnp.exp(jax.random.uniform(jax.random.fold_in(own, position), (parts,), jnp.float32, low / len(pieces), top_value / len(pieces)))
        loudness = loudness * jnp.repeat(heights, shape[position] // parts).reshape([-1 if axis == position else 1 for axis in range(len(shape))])
    return loudness


def bell_draw(own_key, dims, width, reach, pieces=(), held_as=jnp.bfloat16):
    values = width * jax.random.normal(own_key, dims, jnp.float32)
    if pieces:
        values = values * steps_of(own_key, dims, pieces, -0.22, 0.18)
    return jnp.clip(values, -reach, reach).astype(held_as)


def setup_inputs(seed: int = 0) -> dict:
    keys = jax.random.split(jax.random.key(seed), 10)
    solution = bell_draw(keys[0], (FIELDS, NLEV, NLAT, NLON), 1.0, 6.0, ((1, 4), (2, 16), (3, 8)), jnp.float32)
    residual = draw_residual(jax.random.fold_in(keys[9], 71), 0)
    direction = draw_direction(jax.random.fold_in(keys[9], 71), 0)
    ensemble = bell_draw(keys[3], (MEMBERS, VARS, NLEV, NLAT, NLON), 1.0, 6.0, ((2, 4), (3, 16), (4, 8)))
    static_sd = jnp.clip(jnp.exp(math.log(2.0) - 1.3862944 * jax.random.uniform(keys[4], (VARS, NLEV, NLAT, NLON), jnp.float32) ** steps_of(keys[4], (VARS, NLEV, NLAT, NLON), ((1, 4), (2, 16), (3, 8)), -0.2, 0.2)), 0.5, 2.0)
    send_tile = plant(jax.random.randint(keys[5], (N_LEV, N_LON, N_LAT, GROUP, SLOTS), 0, TILES), jax.random.fold_in(keys[5], 1), 0, TILES - 1).astype(jnp.int32)
    pair_count = draw_pair_count(jax.random.fold_in(keys[9], 71), 0)
    obs_weight = bell_draw(keys[7], (N_LEV, N_LON, N_LAT, GROUP, SLOTS, OBS, VARS * CLON), (VARS * CLON) ** -0.5, 0.25, ((0, 4), (1, 8), (2, 16)))
    obs_precision = jnp.clip(jnp.exp(math.log(3000.0) - 3.4011974 * jax.random.uniform(keys[8], (N_LEV, N_LON, N_LAT, GROUP, SLOTS, OBS), jnp.float32) ** steps_of(keys[8], (N_LEV, N_LON, N_LAT, GROUP, SLOTS, OBS), ((0, 4), (1, 8), (2, 16)), -0.2, 0.2)), 100.0, 3000.0)
    return dict(solution=solution, residual=residual, direction=direction, ensemble=ensemble, static_sd=static_sd, send_tile=send_tile, pair_count=pair_count, obs_weight=obs_weight, obs_precision=obs_precision)


spread_lon = 0.075
spread_lat = 0.3
spread_lev = 0.075
ens_share = 0.75
static_part = 0.5


def one_pass(padded):
    centre = padded[:, 1:-1, 1:-1, 1:-1]
    result = centre * (1.0 - 2.0 * (spread_lon + spread_lat + spread_lev))
    result = result + spread_lon * (padded[:, 1:-1, 1:-1, 2:] + padded[:, 1:-1, 1:-1, :-2])
    result = result + spread_lat * (padded[:, 1:-1, 2:, 1:-1] + padded[:, 1:-1, :-2, 1:-1])
    result = result + spread_lev * (padded[:, 2:, 1:-1, 1:-1] + padded[:, :-2, 1:-1, 1:-1])
    return result


def smooth(fields):
    for pass_index in range(4):
        wrapped = jnp.concatenate([fields[:, :, :, -1:], fields, fields[:, :, :, :1]], axis=3)
        padded = jnp.pad(wrapped, ((0, 0), (1, 1), (1, 1), (0, 0)))
        fields = one_pass(padded)
    return fields


def owner_work(operands):
    weights, arrived, precision = operands
    weights_wide = weights.astype(jnp.float32)
    predicted = jnp.einsum("gsbc,gsc->gsb", weights_wide, arrived.astype(jnp.float32))
    weighted = (precision * predicted).astype(jnp.bfloat16)
    return jnp.einsum("gsbc,gsb->gsc", weights_wide, weighted.astype(jnp.float32))


def reference(solution, residual, direction, ensemble, static_sd, send_tile, pair_count, obs_weight, obs_precision):
    scale_ens = (ens_share / MEMBERS) ** 0.5
    tile_width = VARS * CLON
    start_norm = jnp.sum(residual * residual)
    smoothed = smooth(direction)
    ens_part = jnp.sum(ensemble.astype(jnp.float32) * smoothed[:MEMBERS, None], axis=0)
    increment = (scale_ens * ens_part + static_part * static_sd * smoothed[MEMBERS:]).astype(jnp.bfloat16)
    blocks = increment.reshape(VARS, N_LEV, CLEV, N_LAT, CLAT, N_LON, CLON)
    tile_table = blocks.transpose(1, 5, 3, 2, 4, 0, 6).reshape(N_LEV, N_LON, N_LAT, TILES, tile_width)
    tile_pick = send_tile.reshape(N_LEV, N_LON, N_LAT, GROUP * SLOTS).astype(jnp.int32)
    outgoing = jnp.take_along_axis(tile_table, tile_pick[:, :, :, :, None], axis=3)
    is_live = jnp.arange(SLOTS, dtype=jnp.int32)[None, None, None, None, :] < pair_count[:, :, :, :, None]
    is_live = is_live.reshape(N_LEV, N_LON, N_LAT, GROUP * SLOTS)
    outgoing = jnp.where(is_live[:, :, :, :, None], outgoing, jnp.zeros_like(outgoing))
    outgoing = outgoing.reshape(N_LEV, GROUP, GROUP, SLOTS, tile_width)
    arrived = jnp.swapaxes(outgoing, 1, 2).reshape(N_LEV * GROUP, GROUP, SLOTS, tile_width)
    weights = obs_weight.reshape(N_LEV * GROUP, GROUP, SLOTS, OBS, tile_width)
    precision = obs_precision.reshape(N_LEV * GROUP, GROUP, SLOTS, OBS)
    returned = lax.map(owner_work, (weights, arrived, precision))
    returned = jnp.swapaxes(returned.reshape(N_LEV, GROUP, GROUP, SLOTS, tile_width), 1, 2)
    returned = returned.reshape(N_LEV, N_LON, N_LAT, GROUP * SLOTS, tile_width)
    one_hot = (tile_pick[:, :, :, :, None] == jnp.arange(TILES, dtype=jnp.int32)).astype(jnp.float32)
    adj_tiles = jnp.einsum("lopt,lopc->lotc", one_hot.reshape(N_LEV, GROUP, GROUP * SLOTS, TILES), returned.reshape(N_LEV, GROUP, GROUP * SLOTS, tile_width), precision=lax.Precision.HIGHEST)
    adj_tiles = adj_tiles.reshape(N_LEV, N_LON, N_LAT, CLEV, CLAT, VARS, CLON)
    adjoint = adj_tiles.transpose(5, 0, 3, 2, 4, 1, 6).reshape(VARS, NLEV, NLAT, NLON)
    back_ens = scale_ens * jnp.sum(ensemble.astype(jnp.float32) * adjoint[None], axis=1)
    back_static = static_part * static_sd * adjoint
    back = jnp.concatenate([back_ens, back_static], axis=0)
    image_field = direction + smooth(back)
    curvature = jnp.sum(direction * image_field)
    step_size = start_norm / curvature
    new_solution = solution + step_size * direction
    new_residual = residual - step_size * image_field
    next_norm = jnp.sum(new_residual * new_residual)
    new_direction = new_residual + (next_norm / (start_norm + 1e-6)) * direction
    return new_solution, new_residual, new_direction
```

```python
import jax
import jax.numpy as jnp
from jax import lax
from jax.experimental import pallas as pl
from jax.experimental.pallas import tpu as pltpu
from jax.sharding import Mesh
from jax.sharding import PartitionSpec as P

LON = ("lon_0", "lon_1")
LON_LAT = ("lon_0", "lon_1", "lat")


spread_lon = 0.075
spread_lat = 0.3
spread_lev = 0.075
ens_share = 0.75
static_part = 0.5
HALO = 4
VMEM_BYTES = 12 * 1024 * 1024


def shift(x, axis, step):
    devices = lax.axis_size(axis)
    return lax.ppermute(x, axis, [(i, (i + step) % devices) for i in range(devices)])


def total_over(row, axes):
    copies = lax.axis_size(axes)
    rows = jnp.broadcast_to(row[None, :], (copies, row.shape[0]))
    rows = lax.all_to_all(rows, axes, split_axis=0, concat_axis=0, tiled=True)
    return jnp.sum(rows, axis=0)


def pack_kernel(own_ref, north_ref, south_ref, full_ref, first_ref, last_ref):
    groups, fields, planes = own_ref.shape[:3]
    row = lax.broadcasted_iota(jnp.int32, (8, 128), 0)

    def one_field(f, carry):
        rows = []
        for q in range(groups):
            north = north_ref[q, f]
            south = south_ref[q, f]
            for j in range(planes):
                own = pltpu.roll(own_ref[q, f, j], 4, 0)
                above = north if j == 0 else pltpu.roll(north, 4, 0)
                below = pltpu.roll(south, 4, 0) if j == 0 else south
                top = jnp.where(row < 4, above, own)
                bottom = jnp.where(row < 4, own, below)
                full_ref[q, f, j, 0:8] = top
                full_ref[q, f, j, 8:16] = bottom
                rows += [top, bottom]
        columns = jnp.concatenate(rows, axis=0).T
        first_ref[f] = columns[0:8]
        last_ref[f] = columns[120:128]
        return carry

    lax.fori_loop(0, fields, one_field, 0)


def smooth_kernel(place_ref, full_ref, west_ref, east_ref, out_ref):
    groups, fields, planes = full_ref.shape[:3]
    total = groups * planes * 16
    lane = lax.broadcasted_iota(jnp.int32, (total, 128), 1)
    row = lax.broadcasted_iota(jnp.int32, (total, 128), 0) % 16
    sub = lax.broadcasted_iota(jnp.int32, (8, 128), 0)
    low = jnp.where(place_ref[0] == 0, HALO, 0)
    high = jnp.where(place_ref[0] == place_ref[1] - 1, 16 - HALO, 16)
    inside = jnp.where((row >= low) & (row < high), 1.0, 0.0).astype(jnp.float32)
    left_edge = lane == 0
    right_edge = lane == 127
    centre = 1.0 - 2.0 * (spread_lon + spread_lat + spread_lev)
    blank = jnp.zeros((16, 128), jnp.float32)

    def combine(x, beside):
        across = pltpu.roll(x, 1, 0) + pltpu.roll(x, total - 1, 0)
        above = jnp.concatenate([x[16:], blank], axis=0)
        below = jnp.concatenate([blank, x[: total - 16]], axis=0)
        result = centre * x + spread_lon * beside
        result = result + spread_lat * across
        result = result + spread_lev * (above + below)
        return result * inside

    def one_field(f, carry):
        x = full_ref[:, f].reshape(total, 128) * inside
        outer = jnp.concatenate(
            [east_ref[f], jnp.zeros((112, 128), jnp.float32), west_ref[f]], axis=0
        ).T * inside
        for _ in range(4):
            x_left, outer_left = pltpu.roll(x, 1, 1), pltpu.roll(outer, 1, 1)
            x_right, outer_right = pltpu.roll(x, 127, 1), pltpu.roll(outer, 127, 1)
            beside = jnp.where(left_edge, outer_left, x_left) + jnp.where(
                right_edge, outer_right, x_right
            )
            outer_beside = jnp.where(left_edge, x_left, outer_left) + jnp.where(
                right_edge, x_right, outer_right
            )
            x, outer = combine(x, beside), combine(outer, outer_beside)
        for q in range(groups):
            for j in range(planes):
                start = (q * planes + j) * 16
                top = pltpu.roll(x[start : start + 8], 4, 0)
                bottom = pltpu.roll(x[start + 8 : start + 16], 4, 0)
                out_ref[q, f, j] = jnp.where(sub < 4, top, bottom)
        return carry

    lax.fori_loop(0, fields, one_field, 0)


def smooth(fields):
    count, levels, lat_rows, lon_cells = fields.shape
    groups = lax.axis_size("lev")
    share = count // groups
    blocks = fields.reshape(groups, share, levels, lat_rows, lon_cells)
    blocks = lax.all_to_all(blocks, "lev", split_axis=0, concat_axis=0, tiled=True)
    halo_shape = (groups, share, levels * HALO, lon_cells)
    north = shift(blocks[..., lat_rows - HALO :, :].reshape(halo_shape), "lat", 1)
    south = shift(blocks[..., :HALO, :].reshape(halo_shape), "lat", -1)
    strip = jax.ShapeDtypeStruct((share, 8, 128), jnp.float32)
    full, first, last = pl.pallas_call(
        pack_kernel,
        out_shape=(
            jax.ShapeDtypeStruct((groups, share, levels, 16, lon_cells), jnp.float32),
            strip,
            strip,
        ),
        compiler_params=pltpu.CompilerParams(vmem_limit_bytes=VMEM_BYTES),
        name="pack",
    )(blocks, north, south)
    west = shift(last, LON, 1)
    east = shift(first, LON, -1)
    place = jnp.stack([lax.axis_index("lat"), lax.axis_size("lat")]).astype(jnp.int32)
    blocks = pl.pallas_call(
        smooth_kernel,
        out_shape=jax.ShapeDtypeStruct(blocks.shape, jnp.float32),
        in_specs=[pl.BlockSpec(memory_space=pltpu.SMEM)]
        + [pl.BlockSpec(memory_space=pltpu.VMEM)] * 3,
        out_specs=pl.BlockSpec(memory_space=pltpu.VMEM),
        compiler_params=pltpu.CompilerParams(vmem_limit_bytes=VMEM_BYTES),
        name="smooth",
    )(place, full, west, east)
    blocks = lax.all_to_all(blocks, "lev", split_axis=0, concat_axis=0, tiled=True)
    return blocks.reshape(fields.shape)


def body(
    solution,
    residual,
    direction,
    ensemble,
    static_sd,
    send_tile,
    pair_count,
    obs_weight,
    obs_precision,
):
    members, variables, levels, lat_rows, lon_cells = ensemble.shape
    scale_ens = (ens_share / members) ** 0.5
    tile_width = variables * lon_cells
    tile_total = levels * lat_rows
    group_size = send_tile.shape[3]
    slot_count = send_tile.shape[4]
    obs_count = obs_weight.shape[5]
    smoothed = smooth(direction)
    ens_part = jnp.sum(ensemble * smoothed[:members, None], axis=0)
    increment = (scale_ens * ens_part + static_part * static_sd * smoothed[members:]).astype(
        jnp.bfloat16
    )
    tile_table = increment.transpose(1, 2, 0, 3).reshape(tile_total, tile_width)
    tile_pick = send_tile.reshape(group_size * slot_count)
    is_live = (
        jnp.arange(slot_count, dtype=jnp.int32)[None, :] < pair_count.reshape(group_size)[:, None]
    )
    outgoing = jnp.take(tile_table, tile_pick, axis=0)
    outgoing = jnp.where(
        is_live.reshape(group_size * slot_count)[:, None], outgoing, jnp.zeros_like(outgoing)
    )
    outgoing = outgoing.reshape(group_size, slot_count, tile_width)
    arrived = lax.all_to_all(outgoing, LON_LAT, split_axis=0, concat_axis=0, tiled=True)
    weights = obs_weight.reshape(group_size, slot_count, obs_count, tile_width)
    predicted = jnp.einsum("gsbc,gsc->gsb", weights, arrived, preferred_element_type=jnp.float32)
    weighted = (obs_precision.reshape(group_size, slot_count, obs_count) * predicted).astype(
        jnp.bfloat16
    )
    returned = jnp.einsum("gsbc,gsb->gsc", weights, weighted, preferred_element_type=jnp.float32)
    returned = returned.astype(jnp.bfloat16)
    came_back = lax.all_to_all(returned, LON_LAT, split_axis=0, concat_axis=0, tiled=True)
    came_back = came_back.reshape(group_size * slot_count, tile_width)
    one_hot = (tile_pick[:, None] == jnp.arange(tile_total, dtype=jnp.int32)[None, :]).astype(
        jnp.bfloat16
    )
    adj_tiles = jnp.dot(one_hot.T, came_back, preferred_element_type=jnp.float32)
    adjoint = adj_tiles.reshape(levels, lat_rows, variables, lon_cells).transpose(2, 0, 1, 3)
    back_ens = scale_ens * jnp.sum(ensemble * adjoint[None], axis=1)
    back_static = static_part * static_sd * adjoint
    back = jnp.concatenate([back_ens, back_static], axis=0)
    image_field = direction + smooth(back)
    sums = jnp.stack(
        [
            jnp.sum(residual * residual),
            jnp.sum(direction * image_field),
            jnp.sum(residual * image_field),
            jnp.sum(image_field * image_field),
        ]
    )
    sums = total_over(total_over(jnp.pad(sums, (0, 124)), ("lat", "lev")), LON)
    start_norm, curvature, crossed, squared = sums[0], sums[1], sums[2], sums[3]
    step_size = start_norm / curvature
    new_residual = residual - step_size * image_field
    next_norm = start_norm - 2.0 * step_size * crossed + step_size * step_size * squared
    new_solution = solution + step_size * direction
    new_direction = new_residual + next_norm / (start_norm + 1e-06) * direction
    return (new_solution, new_residual, new_direction)


def solution(mesh):
    split = Mesh(
        mesh.devices.reshape(4, 2, mesh.shape["lat"], mesh.shape["lev"]),
        ("lon_0", "lon_1", "lat", "lev"),
    )
    in_specs = (
        P(None, "lev", "lat", LON),
        P(None, "lev", "lat", LON),
        P(None, "lev", "lat", LON),
        P(None, None, "lev", "lat", LON),
        P(None, "lev", "lat", LON),
        P("lev", LON, "lat", None, None),
        P("lev", LON, "lat", None),
        P("lev", LON, "lat", None, None, None, None),
        P("lev", LON, "lat", None, None, None),
    )
    out_specs = (P(None, "lev", "lat", LON), P(None, "lev", "lat", LON), P(None, "lev", "lat", LON))
    return jax.shard_map(body, mesh=split, in_specs=in_specs, out_specs=out_specs, check_vma=False)
```

```python
import jax
import jax.numpy as jnp
from jax import lax
from jax.experimental import pallas as pl
from jax.experimental.pallas import tpu as pltpu
from jax.sharding import Mesh
from jax.sharding import PartitionSpec as P

LON = ("lon_0", "lon_1")
LON_LAT = ("lon_0", "lon_1", "lat")


spread_lon = 0.075
spread_lat = 0.3
spread_lev = 0.075
ens_share = 0.75
static_part = 0.5
HALO = 4
VMEM_BYTES = 12 * 1024 * 1024


def shift(x, axis, step):
    devices = lax.axis_size(axis)
    return lax.ppermute(x, axis, [(i, (i + step) % devices) for i in range(devices)])


def pack_kernel(own_ref, north_ref, south_ref, full_ref, first_ref, last_ref):
    groups, fields, planes = full_ref.shape[:3]
    row = lax.broadcasted_iota(jnp.int32, (8, 128), 0)

    def one_field(f, carry):
        rows = []
        for q in range(groups):
            north = north_ref[q, f]
            south = south_ref[q, f]
            for j in range(planes):
                own = pltpu.roll(own_ref[q, f, j], 4, 0)
                above = north if j == 0 else pltpu.roll(north, 4, 0)
                below = pltpu.roll(south, 4, 0) if j == 0 else south
                top = jnp.where(row < 4, above, own)
                bottom = jnp.where(row < 4, own, below)
                full_ref[q, f, j, 0:8] = top
                full_ref[q, f, j, 8:16] = bottom
                rows += [top, bottom]
        columns = jnp.concatenate(rows, axis=0).T
        first_ref[f] = columns[0:8]
        last_ref[f] = columns[120:128]
        return carry

    lax.fori_loop(0, fields, one_field, 0)


def inside_rows(place_ref, shape, axis):
    row = lax.broadcasted_iota(jnp.int32, shape, axis) % 16
    low = jnp.where(place_ref[0] == 0, HALO, 0)
    high = jnp.where(place_ref[0] == place_ref[1] - 1, 16 - HALO, 16)
    return jnp.where((row >= low) & (row < high), 1.0, 0.0).astype(jnp.float32)


centre_part = 1.0 - 2.0 * (spread_lon + spread_lat + spread_lev)


def strip_passes(place_ref, first_ref, last_ref, west_ref, east_ref, near_ref, far_ref):
    shape = first_ref.shape
    sub = lax.broadcasted_iota(jnp.int32, shape, 1)
    lane = lax.broadcasted_iota(jnp.int32, shape, 2)
    inside = inside_rows(place_ref, shape, 2)
    upper = sub >= 4
    left = pltpu.roll(jnp.where(upper, west_ref[...], first_ref[...]), 4, 1) * inside
    right = pltpu.roll(jnp.where(upper, last_ref[...], east_ref[...]), 4, 1) * inside

    def one_pass(x):
        beside = pltpu.roll(x, 1, 1) + pltpu.roll(x, 7, 1)
        across = pltpu.roll(x, 1, 2) + pltpu.roll(x, 127, 2)
        below = jnp.where(lane < 16, 0.0, pltpu.roll(x, 16, 2))
        above = jnp.where(lane >= 112, 0.0, pltpu.roll(x, 112, 2))
        result = centre_part * x + spread_lon * beside
        result = result + spread_lat * across
        result = result + spread_lev * (above + below)
        return result * inside

    near = jnp.zeros(shape, jnp.float32)
    for step in range(4):
        near = jnp.where(sub == 2 * step, pltpu.roll(left, (2 * step - 3) % 8, 1), near)
        if step == 0:
            far_ref[...] = jnp.where(sub == 7, pltpu.roll(right, 3, 1), 0.0)
        else:
            near = jnp.where(sub == 2 * step - 1, pltpu.roll(right, (2 * step - 5) % 8, 1), near)
        if step < 3:
            left, right = one_pass(left), one_pass(right)
    near_ref[...] = near


def field_passes(inside, x, near, far):
    total = x.shape[0]
    lane = lax.broadcasted_iota(jnp.int32, (total, 128), 1)
    left_edge = lane == 0
    right_edge = lane == 127
    blank = jnp.zeros((16, 128), jnp.float32)
    edges = jnp.concatenate([near, jnp.zeros((112, 128), jnp.float32), far], axis=0).T
    x = x * inside
    for step in range(4):
        edge = edges if step == 0 else pltpu.roll(edges, 128 - 2 * step, 1)
        beside = jnp.where(left_edge, edge, pltpu.roll(x, 1, 1)) + jnp.where(
            right_edge, edge, pltpu.roll(x, 127, 1)
        )
        across = pltpu.roll(x, 1, 0) + pltpu.roll(x, total - 1, 0)
        above = jnp.concatenate([x[16:], blank], axis=0)
        below = jnp.concatenate([blank, x[: total - 16]], axis=0)
        result = centre_part * x + spread_lon * beside
        result = result + spread_lat * across
        result = result + spread_lev * (above + below)
        x = result * inside
    return x


def middle_rows(x, plane):
    sub = lax.broadcasted_iota(jnp.int32, (8, 128), 0)
    top = pltpu.roll(x[plane * 16 : plane * 16 + 8], 4, 0)
    bottom = pltpu.roll(x[plane * 16 + 8 : plane * 16 + 16], 4, 0)
    return jnp.where(sub < 4, top, bottom)


def smooth_kernel(
    place_ref, full_ref, first_ref, last_ref, west_ref, east_ref, out_ref, near_ref, far_ref
):
    groups, fields, planes = full_ref.shape[:3]
    total = groups * planes * 16
    strip_passes(place_ref, first_ref, last_ref, west_ref, east_ref, near_ref, far_ref)
    inside = inside_rows(place_ref, (total, 128), 0)

    def one_field(f, carry):
        x = full_ref[:, f].reshape(total, 128)
        x = field_passes(inside, x, near_ref[f], far_ref[f])
        for q in range(groups):
            for j in range(planes):
                out_ref[q, f, j] = middle_rows(x, q * planes + j)
        return carry

    lax.fori_loop(0, fields, one_field, 0)


def image_kernel(
    place_ref,
    full_ref,
    first_ref,
    last_ref,
    west_ref,
    east_ref,
    pair_ref,
    out_ref,
    near_ref,
    far_ref,
):
    groups, fields, planes = full_ref.shape[:3]
    total = groups * planes * 16
    strip_passes(place_ref, first_ref, last_ref, west_ref, east_ref, near_ref, far_ref)
    inside = inside_rows(place_ref, (total, 128), 0)

    def one_field(f, sums):
        x = full_ref[:, f].reshape(total, 128)
        x = field_passes(inside, x, near_ref[f], far_ref[f])
        start_norm, curvature, crossed, squared = sums
        for q in range(groups):
            for j in range(planes):
                direction = pair_ref[q, f, j]
                residual = pair_ref[q, fields + f, j]
                image = direction + middle_rows(x, q * planes + j)
                out_ref[q, f, j] = image
                start_norm = start_norm + residual * residual
                curvature = curvature + direction * image
                crossed = crossed + residual * image
                squared = squared + image * image
        return (start_norm, curvature, crossed, squared)

    zero = jnp.zeros((8, 128), jnp.float32)
    sums = lax.fori_loop(0, fields, one_field, (zero, zero, zero, zero))
    lane = lax.broadcasted_iota(jnp.int32, (8, 128), 1)
    row = zero
    for k in range(4):
        part = jnp.broadcast_to(jnp.sum(sums[k], axis=0, keepdims=True), (8, 128))
        part = part + pltpu.roll(part, 64, 1)
        part = part + pltpu.roll(part, 32, 1)
        row = jnp.where((lane >= 32 * k) & (lane < 32 * k + 32), part, row)
    for q in range(groups):
        out_ref[q, fields, 0] = row
        out_ref[q, fields, 1] = row


def update_kernel(
    rows_ref,
    image_ref,
    solution_ref,
    residual_ref,
    direction_ref,
    new_solution_ref,
    new_residual_ref,
    new_direction_ref,
):
    groups, fields, planes = solution_ref.shape[:3]
    row = jnp.sum(rows_ref[...], axis=0, keepdims=True)
    lane = lax.broadcasted_iota(jnp.int32, (1, 128), 1)
    start_norm, curvature, crossed, squared = (
        jnp.sum(
            jnp.where((lane >= 32 * k) & (lane < 32 * k + 32), row, 0.0), axis=1, keepdims=True
        )
        for k in range(4)
    )
    step_size = start_norm / curvature
    next_norm = start_norm - 2.0 * step_size * crossed + step_size * step_size * squared
    ratio = next_norm / (start_norm + 1e-06)
    step_size = jnp.broadcast_to(step_size, (8, 128))
    ratio = jnp.broadcast_to(ratio, (8, 128))

    def one_field(f, carry):
        for q in range(groups):
            for j in range(planes):
                direction = direction_ref[q, f, j]
                new_residual = residual_ref[q, f, j] - step_size * image_ref[q, f, j]
                new_solution_ref[q, f, j] = solution_ref[q, f, j] + step_size * direction
                new_residual_ref[q, f, j] = new_residual
                new_direction_ref[q, f, j] = new_residual + ratio * direction
        return carry

    lax.fori_loop(0, fields, one_field, 0)


def swap_lev(blocks):
    return lax.all_to_all(blocks, "lev", split_axis=0, concat_axis=0, tiled=True)


def local_call(kernel, out_shape, scalars, name, scratch=()):
    def run(*operands):
        in_specs = [pl.BlockSpec(memory_space=pltpu.SMEM)] * scalars
        in_specs += [pl.BlockSpec(memory_space=pltpu.VMEM)] * (len(operands) - scalars)
        return pl.pallas_call(
            kernel,
            out_shape=out_shape,
            in_specs=in_specs,
            out_specs=jax.tree.map(lambda _: pl.BlockSpec(memory_space=pltpu.VMEM), out_shape),
            scratch_shapes=list(scratch),
            compiler_params=pltpu.CompilerParams(vmem_limit_bytes=VMEM_BYTES),
            name=name,
        )(*operands)

    return run


def smooth(blocks, share, tail=None):
    groups, _, levels, lat_rows, lon_cells = blocks.shape
    own = blocks[:, :share]
    halo_shape = (groups, share, levels * HALO, lon_cells)
    north = shift(own[..., lat_rows - HALO :, :].reshape(halo_shape), "lat", 1)
    south = shift(own[..., :HALO, :].reshape(halo_shape), "lat", -1)
    strip = jax.ShapeDtypeStruct((share, 8, 128), jnp.float32)
    full = jax.ShapeDtypeStruct((groups, share, levels, 16, lon_cells), jnp.float32)
    full, first, last = local_call(pack_kernel, (full, strip, strip), 0, "pack")(
        blocks, north, south
    )
    west = shift(last, LON, 1)
    east = shift(first, LON, -1)
    place = jnp.stack([lax.axis_index("lat"), lax.axis_size("lat")]).astype(jnp.int32)
    scratch = [pltpu.VMEM((share, 8, 128), jnp.float32)] * 2
    operands = (place, full, first, last, west, east)
    shape = [groups, share, levels, lat_rows, lon_cells]
    if tail is None:
        out = jax.ShapeDtypeStruct(tuple(shape), jnp.float32)
        return local_call(smooth_kernel, out, 1, "smooth", scratch)(*operands)
    shape[1] += 1
    out = jax.ShapeDtypeStruct(tuple(shape), jnp.float32)
    return local_call(image_kernel, out, 1, "image", scratch)(*operands, tail)


def body(
    solution,
    residual,
    direction,
    ensemble,
    static_sd,
    send_tile,
    pair_count,
    obs_weight,
    obs_precision,
):
    members, variables, levels, lat_rows, lon_cells = ensemble.shape
    scale_ens = (ens_share / members) ** 0.5
    tile_width = variables * lon_cells
    tile_total = levels * lat_rows
    group_size = send_tile.shape[3]
    slot_count = send_tile.shape[4]
    obs_count = obs_weight.shape[5]
    groups = lax.axis_size("lev")
    share = direction.shape[0] // groups
    grouped = (groups, share, levels, lat_rows, lon_cells)
    pair = swap_lev(
        jnp.concatenate([direction.reshape(grouped), residual.reshape(grouped)], axis=1)
    )
    smoothed = swap_lev(smooth(pair, share)).reshape(direction.shape)
    ens_part = jnp.sum(ensemble * smoothed[:members, None], axis=0)
    increment = (scale_ens * ens_part + static_part * static_sd * smoothed[members:]).astype(
        jnp.bfloat16
    )
    tile_table = increment.transpose(1, 2, 0, 3).reshape(tile_total, tile_width)
    tile_pick = send_tile.reshape(group_size * slot_count)
    is_live = (
        jnp.arange(slot_count, dtype=jnp.int32)[None, :] < pair_count.reshape(group_size)[:, None]
    )
    outgoing = jnp.take(tile_table, tile_pick, axis=0)
    outgoing = jnp.where(
        is_live.reshape(group_size * slot_count)[:, None], outgoing, jnp.zeros_like(outgoing)
    )
    outgoing = outgoing.reshape(group_size, slot_count, tile_width)
    arrived = lax.all_to_all(outgoing, LON_LAT, split_axis=0, concat_axis=0, tiled=True)
    weights = obs_weight.reshape(group_size, slot_count, obs_count, tile_width)
    predicted = jnp.einsum("gsbc,gsc->gsb", weights, arrived, preferred_element_type=jnp.float32)
    weighted = (obs_precision.reshape(group_size, slot_count, obs_count) * predicted).astype(
        jnp.bfloat16
    )
    returned = jnp.einsum("gsbc,gsb->gsc", weights, weighted, preferred_element_type=jnp.float32)
    returned = returned.astype(jnp.bfloat16)
    came_back = lax.all_to_all(returned, LON_LAT, split_axis=0, concat_axis=0, tiled=True)
    came_back = came_back.reshape(group_size * slot_count, tile_width)
    one_hot = (tile_pick[:, None] == jnp.arange(tile_total, dtype=jnp.int32)[None, :]).astype(
        jnp.bfloat16
    )
    adj_tiles = jnp.dot(one_hot.T, came_back, preferred_element_type=jnp.float32)
    adjoint = adj_tiles.reshape(levels, lat_rows, variables, lon_cells).transpose(2, 0, 1, 3)
    back_ens = scale_ens * jnp.sum(ensemble * adjoint[None], axis=1)
    back_static = static_part * static_sd * adjoint
    back = jnp.concatenate([back_ens, back_static], axis=0)
    image = swap_lev(smooth(swap_lev(back.reshape(grouped)), share, pair))
    peers = lax.axis_size(LON_LAT)
    row = jnp.sum(image[:, share, 0, 0, :], axis=0)
    rows = lax.all_to_all(
        jnp.broadcast_to(row, (peers, 1, lon_cells)), LON_LAT, split_axis=0, concat_axis=0, tiled=True
    )
    out = jax.ShapeDtypeStruct(grouped, jnp.float32)
    outs = local_call(update_kernel, (out, out, out), 0, "update")(
        rows.reshape(peers, lon_cells),
        image,
        solution.reshape(grouped),
        residual.reshape(grouped),
        direction.reshape(grouped),
    )
    return tuple(x.reshape(direction.shape) for x in outs)


def solution(mesh):
    split = Mesh(
        mesh.devices.reshape(4, 2, mesh.shape["lat"], mesh.shape["lev"]),
        ("lon_0", "lon_1", "lat", "lev"),
    )
    in_specs = (
        P(None, "lev", "lat", LON),
        P(None, "lev", "lat", LON),
        P(None, "lev", "lat", LON),
        P(None, None, "lev", "lat", LON),
        P(None, "lev", "lat", LON),
        P("lev", LON, "lat", None, None),
        P("lev", LON, "lat", None),
        P("lev", LON, "lat", None, None, None, None),
        P("lev", LON, "lat", None, None, None),
    )
    out_specs = (P(None, "lev", "lat", LON), P(None, "lev", "lat", LON), P(None, "lev", "lat", LON))
    return jax.shard_map(body, mesh=split, in_specs=in_specs, out_specs=out_specs, check_vma=False)
```

```python
import functools

import jax
import jax.numpy as jnp
from jax import lax
from jax.experimental import pallas as pl
from jax.experimental.pallas import tpu as pltpu
from jax.sharding import Mesh
from jax.sharding import PartitionSpec as P

LON = ("lon_0", "lon_1")
LON_LAT = ("lon_0", "lon_1", "lat")


spread_lon = 0.075
spread_lat = 0.3
spread_lev = 0.075
ens_share = 0.75
static_part = 0.5
HALO = 4
VMEM_BYTES = 12 * 1024 * 1024


def shift(x, axis, step):
    devices = lax.axis_size(axis)
    return lax.ppermute(x, axis, [(i, (i + step) % devices) for i in range(devices)])


def pack_kernel(own_ref, north_ref, south_ref, full_ref, first_ref, last_ref):
    groups, fields, planes = full_ref.shape[:3]
    row = lax.broadcasted_iota(jnp.int32, (8, 128), 0)

    def one_field(f, carry):
        rows = []
        for q in range(groups):
            north = north_ref[q, f]
            south = south_ref[q, f]
            for j in range(planes):
                own = pltpu.roll(own_ref[q, f, j], 4, 0)
                above = north if j == 0 else pltpu.roll(north, 4, 0)
                below = pltpu.roll(south, 4, 0) if j == 0 else south
                top = jnp.where(row < 4, above, own)
                bottom = jnp.where(row < 4, own, below)
                full_ref[q, f, j, 0:8] = top
                full_ref[q, f, j, 8:16] = bottom
                rows += [top, bottom]
        columns = jnp.concatenate(rows, axis=0).T
        first_ref[f] = columns[0:8]
        last_ref[f] = columns[120:128]
        return carry

    lax.fori_loop(0, fields, one_field, 0, unroll=3)


def inside_rows(place_ref, shape, axis):
    row = lax.broadcasted_iota(jnp.int32, shape, axis) % 16
    low = jnp.where(place_ref[0] == 0, HALO, 0)
    high = jnp.where(place_ref[0] == place_ref[1] - 1, 16 - HALO, 16)
    return jnp.where((row >= low) & (row < high), 1.0, 0.0).astype(jnp.float32)


centre_part = 1.0 - 2.0 * (spread_lon + spread_lat + spread_lev)


def strip_passes(place_ref, first_ref, last_ref, west_ref, east_ref, near_ref, far_ref):
    shape = first_ref.shape
    sub = lax.broadcasted_iota(jnp.int32, shape, 1)
    lane = lax.broadcasted_iota(jnp.int32, shape, 2)
    inside = inside_rows(place_ref, shape, 2)
    upper = sub >= 4
    left = pltpu.roll(jnp.where(upper, west_ref[...], first_ref[...]), 4, 1) * inside
    right = pltpu.roll(jnp.where(upper, last_ref[...], east_ref[...]), 4, 1) * inside

    def one_pass(x):
        beside = pltpu.roll(x, 1, 1) + pltpu.roll(x, 7, 1)
        across = pltpu.roll(x, 1, 2) + pltpu.roll(x, 127, 2)
        below = jnp.where(lane < 16, 0.0, pltpu.roll(x, 16, 2))
        above = jnp.where(lane >= 112, 0.0, pltpu.roll(x, 112, 2))
        result = centre_part * x + spread_lon * beside
        result = result + spread_lat * across
        result = result + spread_lev * (above + below)
        return result * inside

    near = jnp.zeros(shape, jnp.float32)
    for step in range(4):
        near = jnp.where(sub == 2 * step, pltpu.roll(left, (2 * step - 3) % 8, 1), near)
        if step == 0:
            far_ref[...] = jnp.where(sub == 7, pltpu.roll(right, 3, 1), 0.0)
        else:
            near = jnp.where(sub == 2 * step - 1, pltpu.roll(right, (2 * step - 5) % 8, 1), near)
        if step < 3:
            left, right = one_pass(left), one_pass(right)
    near_ref[...] = near


def field_passes(coefficients, x, near, far):
    planes = len(x) // 2
    lane = lax.broadcasted_iota(jnp.int32, (8, 128), 1)
    sub = lax.broadcasted_iota(jnp.int32, (8, 128), 0)
    left_edge, right_edge = lane == 0, lane == 127
    first_row, last_row = sub == 0, sub == 7
    edges = jnp.concatenate([near, jnp.zeros((112, 128), jnp.float32), far], axis=0).T
    for step in range(4):
        result = []
        for p in range(planes):
            top, bottom = x[2 * p], x[2 * p + 1]
            top_down, bottom_down = pltpu.roll(top, 1, 0), pltpu.roll(bottom, 1, 0)
            top_up, bottom_up = pltpu.roll(top, 7, 0), pltpu.roll(bottom, 7, 0)
            across = (
                top_down + jnp.where(last_row, bottom_up, top_up),
                jnp.where(first_row, top_down, bottom_down) + bottom_up,
            )
            for h in range(2):
                here = x[2 * p + h]
                centre, lon_part, lat_part, lev_part = coefficients[h]
                start = (2 * p + h) * 8
                edge = edges[start : start + 8]
                if step:
                    edge = pltpu.roll(edge, 128 - 2 * step, 1)
                beside = jnp.where(left_edge, edge, pltpu.roll(here, 1, 1)) + jnp.where(
                    right_edge, edge, pltpu.roll(here, 127, 1)
                )
                total = centre * here + lon_part * beside + lat_part * across[h]
                if p == 0:
                    total = total + lev_part * x[2 + h]
                elif p == planes - 1:
                    total = total + lev_part * x[2 * p - 2 + h]
                else:
                    total = total + lev_part * (x[2 * p - 2 + h] + x[2 * p + 2 + h])
                result.append(total)
        x = result
    return x


def coefficients_of(place_ref):
    halves = []
    for h in range(2):
        row = lax.broadcasted_iota(jnp.int32, (8, 128), 0) + 8 * h
        low = jnp.where(place_ref[0] == 0, HALO, 0)
        high = jnp.where(place_ref[0] == place_ref[1] - 1, 16 - HALO, 16)
        inside = jnp.where((row >= low) & (row < high), 1.0, 0.0).astype(jnp.float32)
        halves.append(
            (inside * centre_part, inside * spread_lon, inside * spread_lat, inside * spread_lev)
        )
    return halves


def field_rows(place_ref, full_ref, f):
    rows = []
    for q in range(full_ref.shape[0]):
        for j in range(full_ref.shape[2]):
            for h in range(2):
                row = lax.broadcasted_iota(jnp.int32, (8, 128), 0) + 8 * h
                low = jnp.where(place_ref[0] == 0, HALO, 0)
                high = jnp.where(place_ref[0] == place_ref[1] - 1, 16 - HALO, 16)
                kept = full_ref[q, f, j, 8 * h : 8 * h + 8]
                rows.append(jnp.where((row >= low) & (row < high), kept, 0.0))
    return rows


def middle_rows(x, plane):
    sub = lax.broadcasted_iota(jnp.int32, (8, 128), 0)
    top = pltpu.roll(x[2 * plane], 4, 0)
    bottom = pltpu.roll(x[2 * plane + 1], 4, 0)
    return jnp.where(sub < 4, top, bottom)


def smooth_kernel(
    place_ref, full_ref, first_ref, last_ref, west_ref, east_ref, out_ref, near_ref, far_ref
):
    groups, fields, planes = full_ref.shape[:3]
    strip_passes(place_ref, first_ref, last_ref, west_ref, east_ref, near_ref, far_ref)
    coefficients = coefficients_of(place_ref)

    def one_field(f, carry):
        x = field_rows(place_ref, full_ref, f)
        x = field_passes(coefficients, x, near_ref[f], far_ref[f])
        for q in range(groups):
            for j in range(planes):
                out_ref[q, f, j] = middle_rows(x, q * planes + j)
        return carry

    lax.fori_loop(0, fields, one_field, 0, unroll=3)


def image_kernel(
    place_ref,
    full_ref,
    first_ref,
    last_ref,
    west_ref,
    east_ref,
    direction_ref,
    pair_ref,
    out_ref,
    near_ref,
    far_ref,
):
    groups, fields, planes = full_ref.shape[:3]
    strip_passes(place_ref, first_ref, last_ref, west_ref, east_ref, near_ref, far_ref)
    coefficients = coefficients_of(place_ref)

    def one_field(f, sums):
        x = field_rows(place_ref, full_ref, f)
        x = field_passes(coefficients, x, near_ref[f], far_ref[f])
        start_norm, curvature, crossed, squared = sums
        for q in range(groups):
            for j in range(planes):
                direction = direction_ref[q, f, j]
                residual = pair_ref[q, fields + f, j]
                image = direction + middle_rows(x, q * planes + j)
                out_ref[q, f, j] = image
                start_norm = start_norm + residual * residual
                curvature = curvature + direction * image
                crossed = crossed + residual * image
                squared = squared + image * image
        return (start_norm, curvature, crossed, squared)

    zero = jnp.zeros((8, 128), jnp.float32)
    sums = lax.fori_loop(0, fields, one_field, (zero, zero, zero, zero), unroll=3)
    lane = lax.broadcasted_iota(jnp.int32, (8, 128), 1)
    row = zero
    for k in range(4):
        part = jnp.broadcast_to(jnp.sum(sums[k], axis=0, keepdims=True), (8, 128))
        part = part + pltpu.roll(part, 64, 1)
        part = part + pltpu.roll(part, 32, 1)
        row = jnp.where((lane >= 32 * k) & (lane < 32 * k + 32), part, row)
    for q in range(groups):
        out_ref[q, fields, 0] = row
        out_ref[q, fields, 1] = row


def update_kernel(
    rows_ref,
    image_ref,
    solution_ref,
    residual_ref,
    direction_ref,
    new_solution_ref,
    new_residual_ref,
    new_direction_ref,
):
    groups, fields, planes = solution_ref.shape[:3]
    row = jnp.sum(rows_ref[...], axis=0, keepdims=True)
    lane = lax.broadcasted_iota(jnp.int32, (1, 128), 1)
    start_norm, curvature, crossed, squared = (
        jnp.sum(
            jnp.where((lane >= 32 * k) & (lane < 32 * k + 32), row, 0.0), axis=1, keepdims=True
        )
        for k in range(4)
    )
    step_size = start_norm / curvature
    next_norm = start_norm - 2.0 * step_size * crossed + step_size * step_size * squared
    ratio = next_norm / (start_norm + 1e-06)
    step_size = jnp.broadcast_to(step_size, (8, 128))
    ratio = jnp.broadcast_to(ratio, (8, 128))

    def one_field(f, carry):
        for q in range(groups):
            for j in range(planes):
                direction = direction_ref[q, f, j]
                new_residual = residual_ref[q, f, j] - step_size * image_ref[q, f, j]
                new_solution_ref[q, f, j] = solution_ref[q, f, j] + step_size * direction
                new_residual_ref[q, f, j] = new_residual
                new_direction_ref[q, f, j] = new_residual + ratio * direction
        return carry

    lax.fori_loop(0, fields, one_field, 0, unroll=3)


def tiles_kernel(scales, smoothed_ref, ensemble_ref, static_sd_ref, chosen_ref, out_ref):
    members, variables, planes = ensemble_ref.shape[:3]
    scale_ens, scale_static = scales
    tiles = []
    for v in range(variables):
        for j in range(planes):
            parts = []
            for k in range(members):
                part = ensemble_ref[k, v, j].astype(jnp.float32) * smoothed_ref[k, j]
                if k < 4:
                    parts.append(part)
                else:
                    parts[k % 4] = parts[k % 4] + part
            ens_part = (parts[0] + parts[1]) + (parts[2] + parts[3])
            static = static_sd_ref[v, j] * smoothed_ref[members + v, j]
            tiles.append(scale_ens * ens_part + scale_static * static)
    tiles = jnp.concatenate(tiles, axis=0).astype(jnp.bfloat16)
    picked = jnp.dot(chosen_ref[...], tiles, preferred_element_type=jnp.float32)
    out_ref[...] = picked.astype(jnp.bfloat16)


def back_kernel(
    scales, came_back_ref, chosen_ref, ensemble_ref, static_sd_ref, residual_ref, out_ref
):
    members, variables, planes = ensemble_ref.shape[:3]
    share = out_ref.shape[1] // 2
    scale_ens, scale_static = scales
    adjoint = lax.dot_general(
        chosen_ref[...],
        came_back_ref[...],
        (((0,), (0,)), ((), ())),
        preferred_element_type=jnp.float32,
    )

    def part(v, j):
        start = (v * planes + j) * 8
        return adjoint[start : start + 8]

    for k in range(members + variables):
        q, f = divmod(k, share)
        for j in range(planes):
            if k < members:
                total = ensemble_ref[k, 0, j].astype(jnp.float32) * part(0, j)
                for v in range(1, variables):
                    total = total + ensemble_ref[k, v, j].astype(jnp.float32) * part(v, j)
                out_ref[q, f, j] = scale_ens * total
            else:
                v = k - members
                out_ref[q, f, j] = scale_static * static_sd_ref[v, j] * part(v, j)
            out_ref[q, share + f, j] = residual_ref[k, j]


def swap_lev(blocks):
    return lax.all_to_all(blocks, "lev", split_axis=0, concat_axis=0, tiled=True)


def local_call(kernel, out_shape, scalars, name, scratch=()):
    def run(*operands):
        in_specs = [pl.BlockSpec(memory_space=pltpu.SMEM)] * scalars
        in_specs += [pl.BlockSpec(memory_space=pltpu.VMEM)] * (len(operands) - scalars)
        return pl.pallas_call(
            kernel,
            out_shape=out_shape,
            in_specs=in_specs,
            out_specs=jax.tree.map(lambda _: pl.BlockSpec(memory_space=pltpu.VMEM), out_shape),
            scratch_shapes=list(scratch),
            compiler_params=pltpu.CompilerParams(vmem_limit_bytes=VMEM_BYTES),
            name=name,
        )(*operands)

    return run


def smooth(blocks, share, tail=None):
    groups, _, levels, lat_rows, lon_cells = blocks.shape
    own = blocks[:, :share]
    halo_shape = (groups, share, levels * HALO, lon_cells)
    north = shift(own[..., lat_rows - HALO :, :].reshape(halo_shape), "lat", 1)
    south = shift(own[..., :HALO, :].reshape(halo_shape), "lat", -1)
    strip = jax.ShapeDtypeStruct((share, 8, 128), jnp.float32)
    full = jax.ShapeDtypeStruct((groups, share, levels, 16, lon_cells), jnp.float32)
    full, first, last = local_call(pack_kernel, (full, strip, strip), 0, "pack")(
        blocks, north, south
    )
    west = shift(last, LON, 1)
    east = shift(first, LON, -1)
    place = jnp.stack([lax.axis_index("lat"), lax.axis_size("lat")]).astype(jnp.int32)
    scratch = [pltpu.VMEM((share, 8, 128), jnp.float32)] * 2
    operands = (place, full, first, last, west, east)
    shape = [groups, share, levels, lat_rows, lon_cells]
    if tail is None:
        out = jax.ShapeDtypeStruct(tuple(shape), jnp.float32)
        return local_call(smooth_kernel, out, 1, "smooth", scratch)(*operands)
    shape[1] += 1
    out = jax.ShapeDtypeStruct(tuple(shape), jnp.float32)
    return local_call(image_kernel, out, 1, "image", scratch)(*operands, *tail)


def body(
    solution,
    residual,
    direction,
    ensemble,
    static_sd,
    send_tile,
    pair_count,
    obs_weight,
    obs_precision,
):
    members, variables, levels, lat_rows, lon_cells = ensemble.shape
    scale_ens = (ens_share / members) ** 0.5
    tile_width = variables * lon_cells
    tile_total = levels * lat_rows
    group_size = send_tile.shape[3]
    slot_count = send_tile.shape[4]
    obs_count = obs_weight.shape[5]
    groups = lax.axis_size("lev")
    share = direction.shape[0] // groups
    grouped = (groups, share, levels, lat_rows, lon_cells)
    direction_blocks = swap_lev(direction.reshape(grouped))
    smoothed = swap_lev(smooth(direction_blocks, share)).reshape(direction.shape)
    tile_pick = send_tile.reshape(group_size, 1, slot_count)
    is_live = (
        jnp.arange(slot_count, dtype=jnp.int32)[None, :] < pair_count.reshape(group_size)[:, None]
    )
    row_pick = jnp.arange(variables, dtype=jnp.int32)[None, :, None] * tile_total + tile_pick
    row_pick = jnp.where(is_live[:, None, :], row_pick, -1)
    row_pick = row_pick.reshape(group_size * variables * slot_count)
    chosen = row_pick[:, None] == jnp.arange(variables * tile_total, dtype=jnp.int32)[None, :]
    chosen = chosen.astype(jnp.bfloat16)
    scales = (scale_ens, static_part)
    rows = jax.ShapeDtypeStruct((group_size * variables * slot_count, lon_cells), jnp.bfloat16)
    outgoing = local_call(functools.partial(tiles_kernel, scales), rows, 0, "tiles")(
        smoothed, ensemble, static_sd, chosen
    )
    block_shape = (group_size, variables, slot_count, lon_cells)
    outgoing = outgoing.reshape(block_shape).transpose(0, 2, 1, 3)
    outgoing = outgoing.reshape(group_size, slot_count, tile_width)
    arrived = lax.all_to_all(outgoing, LON_LAT, split_axis=0, concat_axis=0, tiled=True)
    weights = obs_weight.reshape(group_size, slot_count, obs_count, tile_width)
    predicted = jnp.einsum("gsbc,gsc->gsb", weights, arrived, preferred_element_type=jnp.float32)
    weighted = (obs_precision.reshape(group_size, slot_count, obs_count) * predicted).astype(
        jnp.bfloat16
    )
    returned = jnp.einsum("gsbc,gsb->gsc", weights, weighted, preferred_element_type=jnp.float32)
    returned = returned.astype(jnp.bfloat16)
    came_back = lax.all_to_all(returned, LON_LAT, split_axis=0, concat_axis=0, tiled=True)
    came_back = came_back.reshape(group_size, slot_count, variables, lon_cells)
    came_back = came_back.transpose(0, 2, 1, 3).reshape(-1, lon_cells)
    paired = jax.ShapeDtypeStruct((groups, 2 * share, levels, lat_rows, lon_cells), jnp.float32)
    pair = local_call(functools.partial(back_kernel, scales), paired, 0, "back")(
        came_back, chosen, ensemble, static_sd, residual
    )
    pair = swap_lev(pair)
    image = swap_lev(smooth(pair, share, (direction_blocks, pair)))
    peers = lax.axis_size(LON_LAT)
    row = jnp.sum(image[:, share, 0, 0, :], axis=0)
    rows = lax.all_to_all(
        jnp.broadcast_to(row, (peers, 1, lon_cells)), LON_LAT, split_axis=0, concat_axis=0, tiled=True
    )
    out = jax.ShapeDtypeStruct(grouped, jnp.float32)
    outs = local_call(update_kernel, (out, out, out), 0, "update")(
        rows.reshape(peers, lon_cells),
        image,
        solution.reshape(grouped),
        residual.reshape(grouped),
        direction.reshape(grouped),
    )
    return tuple(x.reshape(direction.shape) for x in outs)


def solution(mesh):
    split = Mesh(
        mesh.devices.reshape(4, 2, mesh.shape["lat"], mesh.shape["lev"]),
        ("lon_0", "lon_1", "lat", "lev"),
    )
    in_specs = (
        P(None, "lev", "lat", LON),
        P(None, "lev", "lat", LON),
        P(None, "lev", "lat", LON),
        P(None, None, "lev", "lat", LON),
        P(None, "lev", "lat", LON),
        P("lev", LON, "lat", None, None),
        P("lev", LON, "lat", None),
        P("lev", LON, "lat", None, None, None, None),
        P("lev", LON, "lat", None, None, None),
    )
    out_specs = (P(None, "lev", "lat", LON), P(None, "lev", "lat", LON), P(None, "lev", "lat", LON))
    return jax.shard_map(body, mesh=split, in_specs=in_specs, out_specs=out_specs, check_vma=False)
```

```python
import functools

import jax
import jax.numpy as jnp
from jax import lax
from jax.experimental import pallas as pl
from jax.experimental.pallas import tpu as pltpu
from jax.sharding import Mesh
from jax.sharding import PartitionSpec as P

LON = ("lon_0", "lon_1")
LON_LAT = ("lon_0", "lon_1", "lat")


spread_lon = 0.075
spread_lat = 0.3
spread_lev = 0.075
ens_share = 0.75
static_part = 0.5
HALO = 4
VMEM_BYTES = 12 * 1024 * 1024


def shift(x, axis, step):
    devices = lax.axis_size(axis)
    return lax.ppermute(x, axis, [(i, (i + step) % devices) for i in range(devices)])


def pack_kernel(own_ref, north_ref, south_ref, full_ref, first_ref, last_ref):
    groups, fields, planes = full_ref.shape[:3]
    row = lax.broadcasted_iota(jnp.int32, (8, 128), 0)

    def one_field(f, carry):
        rows = []
        for q in range(groups):
            north = north_ref[q, f].astype(jnp.float32)
            south = south_ref[q, f].astype(jnp.float32)
            for j in range(planes):
                own = pltpu.roll(own_ref[q, f, j].astype(jnp.float32), 4, 0)
                above = north if j == 0 else pltpu.roll(north, 4, 0)
                below = pltpu.roll(south, 4, 0) if j == 0 else south
                top = jnp.where(row < 4, above, own)
                bottom = jnp.where(row < 4, own, below)
                full_ref[q, f, j, 0:8] = top
                full_ref[q, f, j, 8:16] = bottom
                rows += [top, bottom]
        columns = jnp.concatenate(rows, axis=0).T
        first_ref[f] = columns[0:8]
        last_ref[f] = columns[120:128]
        return carry

    lax.fori_loop(0, fields, one_field, 0, unroll=3)


def inside_rows(place_ref, shape, axis):
    row = lax.broadcasted_iota(jnp.int32, shape, axis) % 16
    low = jnp.where(place_ref[0] == 0, HALO, 0)
    high = jnp.where(place_ref[0] == place_ref[1] - 1, 16 - HALO, 16)
    return jnp.where((row >= low) & (row < high), 1.0, 0.0).astype(jnp.float32)


centre_part = 1.0 - 2.0 * (spread_lon + spread_lat + spread_lev)


def strip_passes(place_ref, first_ref, last_ref, west_ref, east_ref, near_ref, far_ref):
    shape = first_ref.shape
    sub = lax.broadcasted_iota(jnp.int32, shape, 1)
    lane = lax.broadcasted_iota(jnp.int32, shape, 2)
    inside = inside_rows(place_ref, shape, 2)
    upper = sub >= 4
    left = pltpu.roll(jnp.where(upper, west_ref[...], first_ref[...]), 4, 1) * inside
    right = pltpu.roll(jnp.where(upper, last_ref[...], east_ref[...]), 4, 1) * inside

    def one_pass(x):
        beside = pltpu.roll(x, 1, 1) + pltpu.roll(x, 7, 1)
        across = pltpu.roll(x, 1, 2) + pltpu.roll(x, 127, 2)
        below = jnp.where(lane < 16, 0.0, pltpu.roll(x, 16, 2))
        above = jnp.where(lane >= 112, 0.0, pltpu.roll(x, 112, 2))
        result = centre_part * x + spread_lon * beside
        result = result + spread_lat * across
        result = result + spread_lev * (above + below)
        return result * inside

    near = jnp.zeros(shape, jnp.float32)
    for step in range(4):
        near = jnp.where(sub == 2 * step, pltpu.roll(left, (2 * step - 3) % 8, 1), near)
        if step == 0:
            far_ref[...] = jnp.where(sub == 7, pltpu.roll(right, 3, 1), 0.0)
        else:
            near = jnp.where(sub == 2 * step - 1, pltpu.roll(right, (2 * step - 5) % 8, 1), near)
        if step < 3:
            left, right = one_pass(left), one_pass(right)
    near_ref[...] = near


def field_passes(coefficients, x, near, far):
    planes = len(x) // 2
    lane = lax.broadcasted_iota(jnp.int32, (8, 128), 1)
    sub = lax.broadcasted_iota(jnp.int32, (8, 128), 0)
    left_edge, right_edge = lane == 0, lane == 127
    first_row, last_row = sub == 0, sub == 7
    edges = jnp.concatenate([near, jnp.zeros((112, 128), jnp.float32), far], axis=0).T
    for step in range(4):
        result = []
        for p in range(planes):
            top, bottom = x[2 * p], x[2 * p + 1]
            top_down, bottom_down = pltpu.roll(top, 1, 0), pltpu.roll(bottom, 1, 0)
            top_up, bottom_up = pltpu.roll(top, 7, 0), pltpu.roll(bottom, 7, 0)
            across = (
                top_down + jnp.where(last_row, bottom_up, top_up),
                jnp.where(first_row, top_down, bottom_down) + bottom_up,
            )
            for h in range(2):
                here = x[2 * p + h]
                centre, lon_part, lat_part, lev_part = coefficients[h]
                start = (2 * p + h) * 8
                edge = edges[start : start + 8]
                if step:
                    edge = pltpu.roll(edge, 128 - 2 * step, 1)
                beside = jnp.where(left_edge, edge, pltpu.roll(here, 1, 1)) + jnp.where(
                    right_edge, edge, pltpu.roll(here, 127, 1)
                )
                total = centre * here + lon_part * beside + lat_part * across[h]
                if p == 0:
                    total = total + lev_part * x[2 + h]
                elif p == planes - 1:
                    total = total + lev_part * x[2 * p - 2 + h]
                else:
                    total = total + lev_part * (x[2 * p - 2 + h] + x[2 * p + 2 + h])
                result.append(total)
        x = result
    return x


def coefficients_of(place_ref):
    halves = []
    for h in range(2):
        row = lax.broadcasted_iota(jnp.int32, (8, 128), 0) + 8 * h
        low = jnp.where(place_ref[0] == 0, HALO, 0)
        high = jnp.where(place_ref[0] == place_ref[1] - 1, 16 - HALO, 16)
        inside = jnp.where((row >= low) & (row < high), 1.0, 0.0).astype(jnp.float32)
        halves.append(
            (inside * centre_part, inside * spread_lon, inside * spread_lat, inside * spread_lev)
        )
    return halves


def field_rows(place_ref, full_ref, f):
    rows = []
    for q in range(full_ref.shape[0]):
        for j in range(full_ref.shape[2]):
            for h in range(2):
                row = lax.broadcasted_iota(jnp.int32, (8, 128), 0) + 8 * h
                low = jnp.where(place_ref[0] == 0, HALO, 0)
                high = jnp.where(place_ref[0] == place_ref[1] - 1, 16 - HALO, 16)
                kept = full_ref[q, f, j, 8 * h : 8 * h + 8]
                rows.append(jnp.where((row >= low) & (row < high), kept, 0.0))
    return rows


def middle_rows(x, plane):
    sub = lax.broadcasted_iota(jnp.int32, (8, 128), 0)
    top = pltpu.roll(x[2 * plane], 4, 0)
    bottom = pltpu.roll(x[2 * plane + 1], 4, 0)
    return jnp.where(sub < 4, top, bottom)


def smooth_kernel(
    place_ref, full_ref, first_ref, last_ref, west_ref, east_ref, out_ref, near_ref, far_ref
):
    groups, fields, planes = full_ref.shape[:3]
    strip_passes(place_ref, first_ref, last_ref, west_ref, east_ref, near_ref, far_ref)
    coefficients = coefficients_of(place_ref)

    def one_field(f, carry):
        x = field_rows(place_ref, full_ref, f)
        x = field_passes(coefficients, x, near_ref[f], far_ref[f])
        for q in range(groups):
            for j in range(planes):
                out_ref[q, f, j] = middle_rows(x, q * planes + j)
        return carry

    lax.fori_loop(0, fields, one_field, 0, unroll=3)


def image_kernel(
    place_ref,
    full_ref,
    first_ref,
    last_ref,
    west_ref,
    east_ref,
    direction_ref,
    pair_ref,
    out_ref,
    near_ref,
    far_ref,
):
    groups, fields, planes = full_ref.shape[:3]
    strip_passes(place_ref, first_ref, last_ref, west_ref, east_ref, near_ref, far_ref)
    coefficients = coefficients_of(place_ref)

    def one_field(f, sums):
        x = field_rows(place_ref, full_ref, f)
        x = field_passes(coefficients, x, near_ref[f], far_ref[f])
        start_norm, curvature, crossed, squared = sums
        for q in range(groups):
            for j in range(planes):
                direction = direction_ref[q, f, j]
                residual = pair_ref[q, fields + f, j].astype(jnp.float32)
                image = direction + middle_rows(x, q * planes + j)
                out_ref[q, f, j] = image
                start_norm = start_norm + residual * residual
                curvature = curvature + direction * image
                crossed = crossed + residual * image
                squared = squared + image * image
        return (start_norm, curvature, crossed, squared)

    zero = jnp.zeros((8, 128), jnp.float32)
    sums = lax.fori_loop(0, fields, one_field, (zero, zero, zero, zero), unroll=3)
    lane = lax.broadcasted_iota(jnp.int32, (8, 128), 1)
    row = zero
    for k in range(4):
        part = jnp.broadcast_to(jnp.sum(sums[k], axis=0, keepdims=True), (8, 128))
        part = part + pltpu.roll(part, 64, 1)
        part = part + pltpu.roll(part, 32, 1)
        row = jnp.where((lane >= 32 * k) & (lane < 32 * k + 32), part, row)
    for q in range(groups):
        out_ref[q, fields, 0] = row
        out_ref[q, fields, 1] = row


def update_kernel(
    rows_ref,
    image_ref,
    solution_ref,
    residual_ref,
    direction_ref,
    new_solution_ref,
    new_residual_ref,
    new_direction_ref,
):
    groups, fields, planes = solution_ref.shape[:3]
    row = jnp.sum(rows_ref[...], axis=0, keepdims=True)
    lane = lax.broadcasted_iota(jnp.int32, (1, 128), 1)
    start_norm, curvature, crossed, squared = (
        jnp.sum(
            jnp.where((lane >= 32 * k) & (lane < 32 * k + 32), row, 0.0), axis=1, keepdims=True
        )
        for k in range(4)
    )
    step_size = start_norm / curvature
    next_norm = start_norm - 2.0 * step_size * crossed + step_size * step_size * squared
    ratio = next_norm / (start_norm + 1e-06)
    step_size = jnp.broadcast_to(step_size, (8, 128))
    ratio = jnp.broadcast_to(ratio, (8, 128))

    def one_field(f, carry):
        for q in range(groups):
            for j in range(planes):
                direction = direction_ref[q, f, j]
                new_residual = residual_ref[q, f, j] - step_size * image_ref[q, f, j]
                new_solution_ref[q, f, j] = solution_ref[q, f, j] + step_size * direction
                new_residual_ref[q, f, j] = new_residual
                new_direction_ref[q, f, j] = new_residual + ratio * direction
        return carry

    lax.fori_loop(0, fields, one_field, 0, unroll=3)


def tiles_kernel(scales, smoothed_ref, ensemble_ref, static_sd_ref, chosen_ref, out_ref):
    members, variables, planes = ensemble_ref.shape[:3]
    scale_ens, scale_static = scales
    tiles = []
    for v in range(variables):
        for j in range(planes):
            parts = []
            for k in range(members):
                part = ensemble_ref[k, v, j].astype(jnp.float32) * smoothed_ref[k, j]
                if k < 4:
                    parts.append(part)
                else:
                    parts[k % 4] = parts[k % 4] + part
            ens_part = (parts[0] + parts[1]) + (parts[2] + parts[3])
            static = static_sd_ref[v, j] * smoothed_ref[members + v, j]
            tiles.append(scale_ens * ens_part + scale_static * static)
    tiles = jnp.concatenate(tiles, axis=0).astype(jnp.bfloat16)
    picked = jnp.dot(chosen_ref[...], tiles, preferred_element_type=jnp.float32)
    out_ref[...] = picked.astype(jnp.bfloat16)


def back_kernel(
    scales, came_back_ref, chosen_ref, ensemble_ref, static_sd_ref, residual_ref, out_ref
):
    members, variables, planes = ensemble_ref.shape[:3]
    share = out_ref.shape[1] // 2
    scale_ens, scale_static = scales
    adjoint = lax.dot_general(
        chosen_ref[...],
        came_back_ref[...],
        (((0,), (0,)), ((), ())),
        preferred_element_type=jnp.float32,
    )

    def part(v, j):
        start = (v * planes + j) * 8
        return adjoint[start : start + 8]

    for k in range(members + variables):
        q, f = divmod(k, share)
        for j in range(planes):
            if k < members:
                total = ensemble_ref[k, 0, j].astype(jnp.float32) * part(0, j)
                for v in range(1, variables):
                    total = total + ensemble_ref[k, v, j].astype(jnp.float32) * part(v, j)
                out_ref[q, f, j] = (scale_ens * total).astype(jnp.bfloat16)
            else:
                v = k - members
                static = scale_static * static_sd_ref[v, j] * part(v, j)
                out_ref[q, f, j] = static.astype(jnp.bfloat16)
            out_ref[q, share + f, j] = residual_ref[k, j].astype(jnp.bfloat16)


def swap_lev(blocks):
    return lax.all_to_all(blocks, "lev", split_axis=0, concat_axis=0, tiled=True)


def local_call(kernel, out_shape, scalars, name, scratch=()):
    def run(*operands):
        in_specs = [pl.BlockSpec(memory_space=pltpu.SMEM)] * scalars
        in_specs += [pl.BlockSpec(memory_space=pltpu.VMEM)] * (len(operands) - scalars)
        return pl.pallas_call(
            kernel,
            out_shape=out_shape,
            in_specs=in_specs,
            out_specs=jax.tree.map(lambda _: pl.BlockSpec(memory_space=pltpu.VMEM), out_shape),
            scratch_shapes=list(scratch),
            compiler_params=pltpu.CompilerParams(vmem_limit_bytes=VMEM_BYTES),
            name=name,
        )(*operands)

    return run


def smooth(blocks, share, tail=None):
    groups, _, levels, lat_rows, lon_cells = blocks.shape
    own = blocks[:, :share].astype(jnp.bfloat16)
    halo_shape = (groups, share, levels * HALO, lon_cells)
    north = shift(own[..., lat_rows - HALO :, :].reshape(halo_shape), "lat", 1)
    south = shift(own[..., :HALO, :].reshape(halo_shape), "lat", -1)
    strip = jax.ShapeDtypeStruct((share, 8, 128), jnp.float32)
    full = jax.ShapeDtypeStruct((groups, share, levels, 16, lon_cells), jnp.float32)
    full, first, last = local_call(pack_kernel, (full, strip, strip), 0, "pack")(
        blocks, north, south
    )
    west = shift(last, LON, 1)
    east = shift(first, LON, -1)
    place = jnp.stack([lax.axis_index("lat"), lax.axis_size("lat")]).astype(jnp.int32)
    scratch = [pltpu.VMEM((share, 8, 128), jnp.float32)] * 2
    operands = (place, full, first, last, west, east)
    shape = [groups, share, levels, lat_rows, lon_cells]
    if tail is None:
        out = jax.ShapeDtypeStruct(tuple(shape), jnp.float32)
        return local_call(smooth_kernel, out, 1, "smooth", scratch)(*operands)
    shape[1] += 1
    out = jax.ShapeDtypeStruct(tuple(shape), jnp.float32)
    return local_call(image_kernel, out, 1, "image", scratch)(*operands, *tail)


def body(
    solution,
    residual,
    direction,
    ensemble,
    static_sd,
    send_tile,
    pair_count,
    obs_weight,
    obs_precision,
):
    members, variables, levels, lat_rows, lon_cells = ensemble.shape
    scale_ens = (ens_share / members) ** 0.5
    tile_width = variables * lon_cells
    tile_total = levels * lat_rows
    group_size = send_tile.shape[3]
    slot_count = send_tile.shape[4]
    obs_count = obs_weight.shape[5]
    groups = lax.axis_size("lev")
    share = direction.shape[0] // groups
    grouped = (groups, share, levels, lat_rows, lon_cells)
    direction_blocks = swap_lev(direction.reshape(grouped))
    smoothed = swap_lev(smooth(direction_blocks, share)).reshape(direction.shape)
    tile_pick = send_tile.reshape(group_size, 1, slot_count)
    is_live = (
        jnp.arange(slot_count, dtype=jnp.int32)[None, :] < pair_count.reshape(group_size)[:, None]
    )
    row_pick = jnp.arange(variables, dtype=jnp.int32)[None, :, None] * tile_total + tile_pick
    row_pick = jnp.where(is_live[:, None, :], row_pick, -1)
    row_pick = row_pick.reshape(group_size * variables * slot_count)
    chosen = row_pick[:, None] == jnp.arange(variables * tile_total, dtype=jnp.int32)[None, :]
    chosen = chosen.astype(jnp.bfloat16)
    scales = (scale_ens, static_part)
    rows = jax.ShapeDtypeStruct((group_size * variables * slot_count, lon_cells), jnp.bfloat16)
    outgoing = local_call(functools.partial(tiles_kernel, scales), rows, 0, "tiles")(
        smoothed, ensemble, static_sd, chosen
    )
    block_shape = (group_size, variables, slot_count, lon_cells)
    outgoing = outgoing.reshape(block_shape).transpose(0, 2, 1, 3)
    outgoing = outgoing.reshape(group_size, slot_count, tile_width)
    arrived = lax.all_to_all(outgoing, LON_LAT, split_axis=0, concat_axis=0, tiled=True)
    weights = obs_weight.reshape(group_size, slot_count, obs_count, tile_width)
    predicted = jnp.einsum("gsbc,gsc->gsb", weights, arrived, preferred_element_type=jnp.float32)
    weighted = (obs_precision.reshape(group_size, slot_count, obs_count) * predicted).astype(
        jnp.bfloat16
    )
    returned = jnp.einsum("gsbc,gsb->gsc", weights, weighted, preferred_element_type=jnp.float32)
    returned = returned.astype(jnp.bfloat16)
    came_back = lax.all_to_all(returned, LON_LAT, split_axis=0, concat_axis=0, tiled=True)
    came_back = came_back.reshape(group_size, slot_count, variables, lon_cells)
    came_back = came_back.transpose(0, 2, 1, 3).reshape(-1, lon_cells)
    paired = jax.ShapeDtypeStruct((groups, 2 * share, levels, lat_rows, lon_cells), jnp.bfloat16)
    pair = local_call(functools.partial(back_kernel, scales), paired, 0, "back")(
        came_back, chosen, ensemble, static_sd, residual
    )
    pair = swap_lev(pair)
    image = swap_lev(smooth(pair, share, (direction_blocks, pair)))
    peers = lax.axis_size(LON_LAT)
    row = jnp.sum(image[:, share, 0, 0, :], axis=0)
    rows = lax.all_to_all(
        jnp.broadcast_to(row, (peers, 1, lon_cells)), LON_LAT, split_axis=0, concat_axis=0, tiled=True
    )
    out = jax.ShapeDtypeStruct(grouped, jnp.float32)
    outs = local_call(update_kernel, (out, out, out), 0, "update")(
        rows.reshape(peers, lon_cells),
        image,
        solution.reshape(grouped),
        residual.reshape(grouped),
        direction.reshape(grouped),
    )
    return tuple(x.reshape(direction.shape) for x in outs)


def solution(mesh):
    split = Mesh(
        mesh.devices.reshape(4, 2, mesh.shape["lat"], mesh.shape["lev"]),
        ("lon_0", "lon_1", "lat", "lev"),
    )
    in_specs = (
        P(None, "lev", "lat", LON),
        P(None, "lev", "lat", LON),
        P(None, "lev", "lat", LON),
        P(None, None, "lev", "lat", LON),
        P(None, "lev", "lat", LON),
        P("lev", LON, "lat", None, None),
        P("lev", LON, "lat", None),
        P("lev", LON, "lat", None, None, None, None),
        P("lev", LON, "lat", None, None, None),
    )
    out_specs = (P(None, "lev", "lat", LON), P(None, "lev", "lat", LON), P(None, "lev", "lat", LON))
    return jax.shard_map(body, mesh=split, in_specs=in_specs, out_specs=out_specs, check_vma=False)
```

```python
import functools

import jax
import jax.numpy as jnp
from jax import lax
from jax.experimental import pallas as pl
from jax.experimental.pallas import tpu as pltpu
from jax.sharding import Mesh
from jax.sharding import PartitionSpec as P

LON = ("lon_0", "lon_1")
LON_LAT = ("lon_0", "lon_1", "lat")


spread_lon = 0.075
spread_lat = 0.3
spread_lev = 0.075
ens_share = 0.75
static_part = 0.5
HALO = 4
VMEM_BYTES = 12 * 1024 * 1024


def shift(x, axis, step):
    devices = lax.axis_size(axis)
    return lax.ppermute(x, axis, [(i, (i + step) % devices) for i in range(devices)])


def pack_kernel(own_ref, north_ref, south_ref, full_ref, first_ref, last_ref):
    groups, fields, planes = full_ref.shape[:3]
    row = lax.broadcasted_iota(jnp.int32, (8, 128), 0)

    def one_field(f, carry):
        rows = []
        for q in range(groups):
            north = north_ref[q, f]
            south = south_ref[q, f]
            for j in range(planes):
                own = pltpu.roll(own_ref[q, f, j], 4, 0)
                above = north if j == 0 else pltpu.roll(north, 4, 0)
                below = pltpu.roll(south, 4, 0) if j == 0 else south
                top = jnp.where(row < 4, above, own)
                bottom = jnp.where(row < 4, own, below)
                full_ref[q, f, j, 0:8] = top
                full_ref[q, f, j, 8:16] = bottom
                rows += [top, bottom]
        columns = jnp.concatenate(rows, axis=0).T
        first_ref[f] = columns[0:8]
        last_ref[f] = columns[120:128]
        return carry

    lax.fori_loop(0, fields, one_field, 0, unroll=3)


def inside_rows(place_ref, shape, axis):
    row = lax.broadcasted_iota(jnp.int32, shape, axis) % 16
    low = jnp.where(place_ref[0] == 0, HALO, 0)
    high = jnp.where(place_ref[0] == place_ref[1] - 1, 16 - HALO, 16)
    return jnp.where((row >= low) & (row < high), 1.0, 0.0).astype(jnp.float32)


centre_part = 1.0 - 2.0 * (spread_lon + spread_lat + spread_lev)


def strip_passes(place_ref, first_ref, last_ref, west_ref, east_ref, near_ref, far_ref):
    shape = first_ref.shape
    sub = lax.broadcasted_iota(jnp.int32, shape, 1)
    lane = lax.broadcasted_iota(jnp.int32, shape, 2)
    inside = inside_rows(place_ref, shape, 2)
    upper = sub >= 4
    left = pltpu.roll(jnp.where(upper, west_ref[...], first_ref[...]), 4, 1) * inside
    right = pltpu.roll(jnp.where(upper, last_ref[...], east_ref[...]), 4, 1) * inside

    def one_pass(x):
        beside = pltpu.roll(x, 1, 1) + pltpu.roll(x, 7, 1)
        across = pltpu.roll(x, 1, 2) + pltpu.roll(x, 127, 2)
        below = jnp.where(lane < 16, 0.0, pltpu.roll(x, 16, 2))
        above = jnp.where(lane >= 112, 0.0, pltpu.roll(x, 112, 2))
        result = centre_part * x + spread_lon * beside
        result = result + spread_lat * across
        result = result + spread_lev * (above + below)
        return result * inside

    near = jnp.zeros(shape, jnp.float32)
    for step in range(4):
        near = jnp.where(sub == 2 * step, pltpu.roll(left, (2 * step - 3) % 8, 1), near)
        if step == 0:
            far_ref[...] = jnp.where(sub == 7, pltpu.roll(right, 3, 1), 0.0)
        else:
            near = jnp.where(sub == 2 * step - 1, pltpu.roll(right, (2 * step - 5) % 8, 1), near)
        if step < 3:
            left, right = one_pass(left), one_pass(right)
    near_ref[...] = near


lat_ratio = spread_lat / spread_lon
assert spread_lev == spread_lon
centre_ratio = centre_part / spread_lon


def field_passes(coefficients, x, near, far):
    planes = len(x) // 2
    lane = lax.broadcasted_iota(jnp.int32, (8, 128), 1)
    sub = lax.broadcasted_iota(jnp.int32, (8, 128), 0)
    left_edge, right_edge = lane == 0, lane == 127
    first_row, last_row = sub == 0, sub == 7
    edges = jnp.concatenate([near, jnp.zeros((112, 128), jnp.float32), far], axis=0).T
    for step in range(4):
        result = []
        for p in range(planes):
            top, bottom = x[2 * p], x[2 * p + 1]
            top_down, bottom_down = pltpu.roll(top, 1, 0), pltpu.roll(bottom, 1, 0)
            top_up, bottom_up = pltpu.roll(top, 7, 0), pltpu.roll(bottom, 7, 0)
            across = (
                top_down + jnp.where(last_row, bottom_up, top_up),
                jnp.where(first_row, top_down, bottom_down) + bottom_up,
            )
            for h in range(2):
                here = x[2 * p + h]
                start = (2 * p + h) * 8
                edge = edges[start : start + 8]
                if step:
                    edge = pltpu.roll(edge, 128 - 2 * step, 1)
                beside = jnp.where(left_edge, edge, pltpu.roll(here, 1, 1)) + jnp.where(
                    right_edge, edge, pltpu.roll(here, 127, 1)
                )
                if p == 0:
                    beside = beside + x[2 + h]
                elif p == planes - 1:
                    beside = beside + x[2 * p - 2 + h]
                else:
                    beside = beside + (x[2 * p - 2 + h] + x[2 * p + 2 + h])
                total = beside + lat_ratio * across[h]
                total = coefficients[h] * (total + centre_ratio * here)
                result.append(total)
        x = result
    return x


def coefficients_of(place_ref):
    halves = []
    for h in range(2):
        row = lax.broadcasted_iota(jnp.int32, (8, 128), 0) + 8 * h
        low = jnp.where(place_ref[0] == 0, HALO, 0)
        high = jnp.where(place_ref[0] == place_ref[1] - 1, 16 - HALO, 16)
        inside = jnp.where((row >= low) & (row < high), 1.0, 0.0).astype(jnp.float32)
        halves.append(inside * spread_lon)
    return halves


def field_rows(place_ref, full_ref, f):
    rows = []
    for q in range(full_ref.shape[0]):
        for j in range(full_ref.shape[2]):
            for h in range(2):
                row = lax.broadcasted_iota(jnp.int32, (8, 128), 0) + 8 * h
                low = jnp.where(place_ref[0] == 0, HALO, 0)
                high = jnp.where(place_ref[0] == place_ref[1] - 1, 16 - HALO, 16)
                kept = full_ref[q, f, j, 8 * h : 8 * h + 8]
                rows.append(jnp.where((row >= low) & (row < high), kept, 0.0))
    return rows


def middle_rows(x, plane):
    sub = lax.broadcasted_iota(jnp.int32, (8, 128), 0)
    top = pltpu.roll(x[2 * plane], 4, 0)
    bottom = pltpu.roll(x[2 * plane + 1], 4, 0)
    return jnp.where(sub < 4, top, bottom)


def smooth_kernel(
    place_ref, full_ref, first_ref, last_ref, west_ref, east_ref, out_ref, near_ref, far_ref
):
    groups, fields, planes = full_ref.shape[:3]
    strip_passes(place_ref, first_ref, last_ref, west_ref, east_ref, near_ref, far_ref)
    coefficients = coefficients_of(place_ref)

    def one_field(f, carry):
        x = field_rows(place_ref, full_ref, f)
        x = field_passes(coefficients, x, near_ref[f], far_ref[f])
        for q in range(groups):
            for j in range(planes):
                out_ref[q, f, j] = middle_rows(x, q * planes + j)
        return carry

    lax.fori_loop(0, fields, one_field, 0, unroll=3)


def image_kernel(
    place_ref,
    full_ref,
    first_ref,
    last_ref,
    west_ref,
    east_ref,
    direction_ref,
    pair_ref,
    out_ref,
    near_ref,
    far_ref,
):
    groups, fields, planes = full_ref.shape[:3]
    strip_passes(place_ref, first_ref, last_ref, west_ref, east_ref, near_ref, far_ref)
    coefficients = coefficients_of(place_ref)

    def one_field(f, sums):
        x = field_rows(place_ref, full_ref, f)
        x = field_passes(coefficients, x, near_ref[f], far_ref[f])
        start_norm, curvature, crossed, squared = sums
        for q in range(groups):
            for j in range(planes):
                direction = direction_ref[q, f, j]
                residual = pair_ref[q, fields + f, j]
                image = direction + middle_rows(x, q * planes + j)
                out_ref[q, f, j] = image
                start_norm = start_norm + residual * residual
                curvature = curvature + direction * image
                crossed = crossed + residual * image
                squared = squared + image * image
        return (start_norm, curvature, crossed, squared)

    zero = jnp.zeros((8, 128), jnp.float32)
    sums = lax.fori_loop(0, fields, one_field, (zero, zero, zero, zero), unroll=3)
    lane = lax.broadcasted_iota(jnp.int32, (8, 128), 1)
    row = zero
    for k in range(4):
        part = jnp.broadcast_to(jnp.sum(sums[k], axis=0, keepdims=True), (8, 128))
        part = part + pltpu.roll(part, 64, 1)
        part = part + pltpu.roll(part, 32, 1)
        row = jnp.where((lane >= 32 * k) & (lane < 32 * k + 32), part, row)
    for q in range(groups):
        out_ref[q, fields, 0] = row
        out_ref[q, fields, 1] = row


def update_kernel(
    rows_ref,
    image_ref,
    solution_ref,
    residual_ref,
    direction_ref,
    new_solution_ref,
    new_residual_ref,
    new_direction_ref,
):
    groups, fields, planes = solution_ref.shape[:3]
    row = jnp.sum(rows_ref[...], axis=0, keepdims=True)
    lane = lax.broadcasted_iota(jnp.int32, (1, 128), 1)
    start_norm, curvature, crossed, squared = (
        jnp.sum(
            jnp.where((lane >= 32 * k) & (lane < 32 * k + 32), row, 0.0), axis=1, keepdims=True
        )
        for k in range(4)
    )
    step_size = start_norm / curvature
    next_norm = start_norm - 2.0 * step_size * crossed + step_size * step_size * squared
    ratio = next_norm / (start_norm + 1e-06)
    step_size = jnp.broadcast_to(step_size, (8, 128))
    ratio = jnp.broadcast_to(ratio, (8, 128))

    def one_field(f, carry):
        for q in range(groups):
            for j in range(planes):
                direction = direction_ref[q, f, j]
                new_residual = residual_ref[q, f, j] - step_size * image_ref[q, f, j]
                new_solution_ref[q, f, j] = solution_ref[q, f, j] + step_size * direction
                new_residual_ref[q, f, j] = new_residual
                new_direction_ref[q, f, j] = new_residual + ratio * direction
        return carry

    lax.fori_loop(0, fields, one_field, 0, unroll=3)


def tiles_kernel(scales, smoothed_ref, ensemble_ref, static_sd_ref, chosen_ref, out_ref):
    members, variables, planes = ensemble_ref.shape[:3]
    scale_ens, scale_static = scales
    tiles = []
    for v in range(variables):
        for j in range(planes):
            parts = []
            for k in range(members):
                part = ensemble_ref[k, v, j].astype(jnp.float32) * smoothed_ref[k, j]
                if k < 4:
                    parts.append(part)
                else:
                    parts[k % 4] = parts[k % 4] + part
            ens_part = (parts[0] + parts[1]) + (parts[2] + parts[3])
            static = static_sd_ref[v, j] * smoothed_ref[members + v, j]
            tiles.append(scale_ens * ens_part + scale_static * static)
    tiles = jnp.concatenate(tiles, axis=0).astype(jnp.bfloat16)
    picked = jnp.dot(chosen_ref[...], tiles, preferred_element_type=jnp.float32)
    out_ref[...] = picked.astype(jnp.bfloat16)


def back_kernel(
    scales, came_back_ref, chosen_ref, ensemble_ref, static_sd_ref, residual_ref, out_ref
):
    members, variables, planes = ensemble_ref.shape[:3]
    share = out_ref.shape[1] // 2
    scale_ens, scale_static = scales
    adjoint = lax.dot_general(
        chosen_ref[...],
        came_back_ref[...],
        (((0,), (0,)), ((), ())),
        preferred_element_type=jnp.float32,
    )

    def part(v, j):
        start = (v * planes + j) * 8
        return adjoint[start : start + 8]

    for k in range(members + variables):
        q, f = divmod(k, share)
        for j in range(planes):
            if k < members:
                total = ensemble_ref[k, 0, j].astype(jnp.float32) * part(0, j)
                for v in range(1, variables):
                    total = total + ensemble_ref[k, v, j].astype(jnp.float32) * part(v, j)
                out_ref[q, f, j] = scale_ens * total
            else:
                v = k - members
                out_ref[q, f, j] = scale_static * static_sd_ref[v, j] * part(v, j)
            out_ref[q, share + f, j] = residual_ref[k, j]


def swap_lev(blocks):
    return lax.all_to_all(blocks, "lev", split_axis=0, concat_axis=0, tiled=True)


def local_call(kernel, out_shape, scalars, name, scratch=()):
    def run(*operands):
        in_specs = [pl.BlockSpec(memory_space=pltpu.SMEM)] * scalars
        in_specs += [pl.BlockSpec(memory_space=pltpu.VMEM)] * (len(operands) - scalars)
        return pl.pallas_call(
            kernel,
            out_shape=out_shape,
            in_specs=in_specs,
            out_specs=jax.tree.map(lambda _: pl.BlockSpec(memory_space=pltpu.VMEM), out_shape),
            scratch_shapes=list(scratch),
            compiler_params=pltpu.CompilerParams(vmem_limit_bytes=VMEM_BYTES),
            name=name,
        )(*operands)

    return run


def smooth(blocks, share, tail=None):
    groups, _, levels, lat_rows, lon_cells = blocks.shape
    own = blocks[:, :share]
    halo_shape = (groups, share, levels * HALO, lon_cells)
    north = shift(own[..., lat_rows - HALO :, :].reshape(halo_shape), "lat", 1)
    south = shift(own[..., :HALO, :].reshape(halo_shape), "lat", -1)
    strip = jax.ShapeDtypeStruct((share, 8, 128), jnp.float32)
    full = jax.ShapeDtypeStruct((groups, share, levels, 16, lon_cells), jnp.float32)
    full, first, last = local_call(pack_kernel, (full, strip, strip), 0, "pack")(
        blocks, north, south
    )
    west = shift(last, LON, 1)
    east = shift(first, LON, -1)
    place = jnp.stack([lax.axis_index("lat"), lax.axis_size("lat")]).astype(jnp.int32)
    scratch = [pltpu.VMEM((share, 8, 128), jnp.float32)] * 2
    operands = (place, full, first, last, west, east)
    shape = [groups, share, levels, lat_rows, lon_cells]
    if tail is None:
        out = jax.ShapeDtypeStruct(tuple(shape), jnp.float32)
        return local_call(smooth_kernel, out, 1, "smooth", scratch)(*operands)
    shape[1] += 1
    out = jax.ShapeDtypeStruct(tuple(shape), jnp.float32)
    return local_call(image_kernel, out, 1, "image", scratch)(*operands, *tail)


def body(
    solution,
    residual,
    direction,
    ensemble,
    static_sd,
    send_tile,
    pair_count,
    obs_weight,
    obs_precision,
):
    members, variables, levels, lat_rows, lon_cells = ensemble.shape
    scale_ens = (ens_share / members) ** 0.5
    tile_width = variables * lon_cells
    tile_total = levels * lat_rows
    group_size = send_tile.shape[3]
    slot_count = send_tile.shape[4]
    obs_count = obs_weight.shape[5]
    groups = lax.axis_size("lev")
    share = direction.shape[0] // groups
    grouped = (groups, share, levels, lat_rows, lon_cells)
    tile_pick = send_tile.reshape(group_size, 1, slot_count)
    is_live = (
        jnp.arange(slot_count, dtype=jnp.int32)[None, :] < pair_count.reshape(group_size)[:, None]
    )
    row_pick = jnp.arange(variables, dtype=jnp.int32)[None, :, None] * tile_total + tile_pick
    row_pick = jnp.where(is_live[:, None, :], row_pick, -1)
    row_pick = row_pick.reshape(group_size * variables * slot_count)
    chosen = row_pick[:, None] == jnp.arange(variables * tile_total, dtype=jnp.int32)[None, :]
    chosen = chosen.astype(jnp.bfloat16)
    direction_blocks = swap_lev(direction.reshape(grouped))
    direction_blocks, chosen = lax.optimization_barrier((direction_blocks, chosen))
    smoothed = swap_lev(smooth(direction_blocks, share)).reshape(direction.shape)
    scales = (scale_ens, static_part)
    rows = jax.ShapeDtypeStruct((group_size * variables * slot_count, lon_cells), jnp.bfloat16)
    outgoing = local_call(functools.partial(tiles_kernel, scales), rows, 0, "tiles")(
        smoothed, ensemble, static_sd, chosen
    )
    block_shape = (group_size, variables, slot_count, lon_cells)
    outgoing = outgoing.reshape(block_shape).transpose(0, 2, 1, 3)
    outgoing = outgoing.reshape(group_size, slot_count, tile_width)
    arrived = lax.all_to_all(outgoing, LON_LAT, split_axis=0, concat_axis=0, tiled=True)
    weights = obs_weight.reshape(group_size, slot_count, obs_count, tile_width)
    predicted = jnp.einsum("gsbc,gsc->gsb", weights, arrived, preferred_element_type=jnp.float32)
    weighted = (obs_precision.reshape(group_size, slot_count, obs_count) * predicted).astype(
        jnp.bfloat16
    )
    returned = jnp.einsum("gsbc,gsb->gsc", weights, weighted, preferred_element_type=jnp.float32)
    returned = returned.astype(jnp.bfloat16)
    came_back = lax.all_to_all(returned, LON_LAT, split_axis=0, concat_axis=0, tiled=True)
    came_back = came_back.reshape(group_size, slot_count, variables, lon_cells)
    came_back = came_back.transpose(0, 2, 1, 3).reshape(-1, lon_cells)
    paired = jax.ShapeDtypeStruct((groups, 2 * share, levels, lat_rows, lon_cells), jnp.float32)
    pair = local_call(functools.partial(back_kernel, scales), paired, 0, "back")(
        came_back, chosen, ensemble, static_sd, residual
    )
    pair = swap_lev(pair)
    image = swap_lev(smooth(pair, share, (direction_blocks, pair)))
    peers = lax.axis_size(LON_LAT)
    row = jnp.sum(image[:, share, 0, 0, :], axis=0)
    rows = lax.all_to_all(
        jnp.broadcast_to(row, (peers, 1, lon_cells)), LON_LAT, split_axis=0, concat_axis=0, tiled=True
    )
    out = jax.ShapeDtypeStruct(grouped, jnp.float32)
    outs = local_call(update_kernel, (out, out, out), 0, "update")(
        rows.reshape(peers, lon_cells),
        image,
        solution.reshape(grouped),
        residual.reshape(grouped),
        direction.reshape(grouped),
    )
    return tuple(x.reshape(direction.shape) for x in outs)


def solution(mesh):
    split = Mesh(
        mesh.devices.reshape(4, 2, mesh.shape["lat"], mesh.shape["lev"]),
        ("lon_0", "lon_1", "lat", "lev"),
    )
    in_specs = (
        P(None, "lev", "lat", LON),
        P(None, "lev", "lat", LON),
        P(None, "lev", "lat", LON),
        P(None, None, "lev", "lat", LON),
        P(None, "lev", "lat", LON),
        P("lev", LON, "lat", None, None),
        P("lev", LON, "lat", None),
        P("lev", LON, "lat", None, None, None, None),
        P("lev", LON, "lat", None, None, None),
    )
    out_specs = (P(None, "lev", "lat", LON), P(None, "lev", "lat", LON), P(None, "lev", "lat", LON))
    return jax.shard_map(body, mesh=split, in_specs=in_specs, out_specs=out_specs, check_vma=False)
```
